32 devices in a mesh: grp: 4 (over z), tm: 8 (over y, x, core).
Axes of the slice: x: 2, y: 2, z: 4, core: 2. Of those that a mesh axis runs over, the one named last changes fastest.
Arguments:
- initial: float32 [8, 16384], P('grp'), parts along dimension 0, may hold values from -1 to 1
- forcing: float32 [8, 32, 16384], P('grp', 'tm'), parts along dimension 0, may hold values from -1.8 to 1.8
- fine_blocks: float32 [16, 3, 128, 128], replicated, may hold values from -0.2 to 0.9, as said below
- coarse_blocks: float32 [16, 3, 128, 128], replicated, may hold values from -0.2 to 0.9, as said below
Outputs:
- solution: float32 [8, 32, 16384], P('grp', 'tm'), parts along dimension 0
The draws below stay inside these ranges and needn't reach their ends.
There are 4 independent parts, one for each index of `grp`. The reference program is written for one: setup_inputs(seed, part) draws one part's arguments, and reference() takes and returns one part's arrays. A program takes and returns all parts, laid end to end along the dimension named above; an argument that names none is the same for every part. Nothing has to cross between parts.
Inputs may be any that keep to these rules, and one draw needn't show every extreme that they name: `fine_blocks`: 16 x 3 blocks of 128 x 128. `coarse_blocks`: 16 x 3 blocks of 128 x 128.
All inputs are finite; a program needn't handle non-finite values.
Results may differ from the reference program's by a relative error of at most 0.00013.
Values sent between devices are 32-bit elements; how exact they have to be, the bound alone decides.
A program may use at most 64 MiB of HBM per device.

```python
import math
import jax
import jax.numpy as jnp
from jax import lax

W = 16384
BLK = 128
ZONES = 16
INST = 2
M = 4
ITERS = 1
NT = 32


def make_blocks(key, centre):
    noise = jnp.clip(jax.random.normal(key, (ZONES, 3, BLK, BLK), jnp.float32), -4.0, 4.0)
    noise = noise / math.sqrt(BLK)
    weights = jnp.array([0.12, 0.25, 0.12], jnp.float32)[None, :, None, None]
    middle = jnp.array([0.0, 1.0, 0.0], jnp.float32)[None, :, None, None]
    return noise * weights + centre * middle * jnp.eye(BLK, dtype=jnp.float32)[None, None]


def draw_fine_blocks(key, part):
    return make_blocks(jax.random.fold_in(key, 11), 0.7)


def draw_coarse_blocks(key, part):
    return make_blocks(jax.random.fold_in(key, 23), 0.65)


def levels(stream_key, shape, split, low, top_value):
    gain = 1.0
    for position, parts in split:
        steps = jax.random.uniform(jax.random.fold_in(jax.random.fold_in(stream_key, 6), position), (parts,), jnp.float32, low / len(split), top_value / len(split))
        gain = gain * jnp.repeat(jnp.exp(steps), shape[position] // parts).reshape((-1,) + (1,) * (len(shape) - 1 - position))
    return gain


def normal_values(rng, extent, deviation, reach, pieces=(), kind=jnp.bfloat16):
    gain = levels(rng, extent, pieces, -0.22, 0.18) if pieces else 1.0
    values = jax.random.normal(rng, extent, jnp.float32) * deviation * gain
    return jnp.minimum(jnp.maximum(values, -reach), reach).astype(kind)


def setup_inputs(seed: int = 0, part: int = 0) -> dict:
    streams_of = jax.random.split(jax.random.key(seed), 5)
    own_keys = jax.random.split(jax.random.fold_in(streams_of[4], part), 5)
    initial = jnp.clip(jax.random.uniform(own_keys[0], (INST, W), jnp.float32, -1.0, 1.0), -1.0, 1.0)
    forcing = normal_values(own_keys[1], (INST, NT, W), 0.3, 1.8, ((1, 8),), jnp.float32)
    fine_blocks = draw_fine_blocks(jax.random.fold_in(streams_of[4], 71), part)
    coarse_blocks = draw_coarse_blocks(jax.random.fold_in(streams_of[4], 71), part)
    return {"initial": initial, "forcing": forcing, "fine_blocks": fine_blocks, "coarse_blocks": coarse_blocks}


DELTA = 0.05


def propagate(states, blocks, delta_t):
    layout = states.shape
    block_size = blocks.shape[-1]
    zone_count = blocks.shape[0]
    grouped = states.reshape(-1, layout[-1] // block_size, block_size)
    border = jnp.zeros_like(grouped[:, :1])
    left_side = jnp.concatenate([border, grouped[:, :-1]], axis=1)
    right_side = jnp.concatenate([grouped[:, 1:], border], axis=1)
    stacked = jnp.stack([left_side, grouped, right_side]).reshape(3, grouped.shape[0], -1, zone_count, block_size)
    mixing = jnp.einsum("kbrzn,zkmn->brzm", stacked, blocks, precision=lax.Precision.HIGHEST).reshape(layout)
    solved = mixing
    for _ in range(2):
        cubed_part = solved * solved * solved
        solved = solved - (solved - delta_t * (solved - cubed_part) - mixing) / (1.0 - delta_t + 3.0 * delta_t * solved * solved)
    return solved


def sweep(current, forcing_grid, carried, blocks, want_next):
    running = carried
    columns = []
    for slot in range(current.shape[2] - 1):
        running = propagate(running, blocks, DELTA) + forcing_grid[:, :, slot]
        columns.append(running)
    columns.append(current[:, :, -1])
    updated = jnp.stack(columns, axis=2)
    following = propagate(running, blocks, DELTA) + forcing_grid[:, :, -1] if want_next else None
    return updated, following


def coarse_chain(start, rhs_values, blocks, coarse_dt):
    def advance(carry_state, source):
        stepped = propagate(carry_state, blocks, coarse_dt) + source
        return stepped, stepped
    _, history = lax.scan(advance, start, jnp.moveaxis(rhs_values, 1, 0))
    return jnp.moveaxis(history, 0, 1)


def reference(initial, forcing, fine_blocks, coarse_blocks):
    members = forcing.shape[0]
    grid_cells = forcing.shape[2]
    forcing_grid = forcing.reshape(members, -1, M, grid_cells)
    current = jnp.zeros(forcing_grid.shape, jnp.float32)

    def carried_in(values):
        return jnp.concatenate([initial[:, None], values[:, :-1, -1]], axis=1)

    current, _ = sweep(current, forcing_grid, carried_in(current), fine_blocks, False)
    for _ in range(ITERS):
        corner = propagate(current[:, :, -2], fine_blocks, DELTA) + forcing_grid[:, :, -1]
        current = jnp.concatenate([current[:, :, :-1], corner[:, :, None]], axis=2)
        carried = carried_in(current)
        current, following = sweep(current, forcing_grid, carried, fine_blocks, True)
        coarse_rhs = following - propagate(carried, coarse_blocks, DELTA * M)
        coarse_vals = coarse_chain(initial, coarse_rhs, coarse_blocks, DELTA * M)
        current = jnp.concatenate([current[:, :, :-1], coarse_vals[:, :, None]], axis=2)
        current, _ = sweep(current, forcing_grid, carried_in(current), fine_blocks, False)
    return current.reshape(members, -1, grid_cells)
```

```python
import functools

import jax
import jax.numpy as jnp
from jax import lax
from jax.experimental import pallas as pl
from jax.experimental.pallas import tpu as pltpu
from jax.sharding import PartitionSpec as P

M = 4
DELTA = 0.05
MESH = pl.DeviceIdType.MESH
F8 = jnp.float8_e4m3fn


def newton(mixing, delta_t):
    solved = mixing
    for _ in range(2):
        squared = solved * solved
        solved = (mixing + (2.0 * delta_t) * solved * squared) / (
            (1.0 - delta_t) + (3.0 * delta_t) * squared
        )
    return solved


LIFT = 65536.0


def kernel(
    n, inst, zones, reps, pieces,
    init_hbm, forc_hbm, fine_hbm, coarse_hbm, out_ref,
    init_ref, forc_ref, raw, wide, fix, x, ubuf, carr, rbuf, pbuf,
    load_sem, state_sem, carr_send, carr_recv, r_send, r_recv, fwd_send,
):
    me = lax.axis_index("tm")
    blk = raw.shape[-1]
    rows = inst * reps
    coarse_dt = DELTA * M
    part = zones // pieces
    pairs = zones // 2
    odd = lax.rem(me, 2)

    def load(which, c):
        span = pl.ds(c * part, part)
        return pltpu.make_async_copy((fine_hbm, coarse_hbm)[which].at[span], raw.at[which, span], load_sem.at[which, c])

    state_loads = [
        pltpu.make_async_copy(init_hbm, init_ref, state_sem.at[0]),
        pltpu.make_async_copy(forc_hbm, forc_ref, state_sem.at[1]),
    ]
    for c in range(pieces):
        load(0, c).start()
    for copy in state_loads:
        copy.start()

    barrier = pltpu.get_barrier_semaphore()
    for step in range(1, n):
        pl.semaphore_signal(barrier, inc=1, device_id={"tm": lax.rem(me + step, n)}, device_id_type=MESH)

    def initial_at(z):
        return jnp.concatenate(
            [init_ref[pl.ds(z * inst + i, reps, stride=zones * inst), :] for i in range(inst)], axis=0
        )

    def forcing_at(slot, z):
        return jnp.concatenate(
            [forc_ref[pl.ds((i * reps * zones + z) * M + slot, reps, stride=zones * M), :] for i in range(inst)],
            axis=0,
        )

    def emit_out(slot, z, value):
        for i in range(inst):
            out_ref[pl.ds((i * reps * zones + z) * M + slot, reps, stride=zones * M), :] = value[
                i * reps : (i + 1) * reps
            ]

    row = lax.broadcasted_iota(jnp.int32, (rows, blk), 0)

    def put(dst, z, value):
        def write(slot, v):
            high = v.astype(jnp.bfloat16)
            low = (v - high.astype(jnp.float32)).astype(jnp.bfloat16)
            x[dst, slot, :rows] = high
            x[dst, slot, rows:] = low

        write(z + 1, value)
        if z == 0:
            rolled = pltpu.roll(value, rows - 1, 0)
            write(zones + 1, jnp.where(row % reps == reps - 1, 0.0, rolled))
        if z == zones - 1:
            rolled = pltpu.roll(value, 1, 0)
            write(0, jnp.where(row % reps == 0, 0.0, rolled))

    def propagate(src, which, delta_t, emit, turn=0):
        for q in range(pairs):
            p = (q + turn) % pairs
            z = 2 * p

            def left(i, stop):
                return jnp.concatenate([x[src, z + i + k, :stop] for k in range(3)], axis=1)

            main = jnp.dot(
                jnp.concatenate([left(0, 2 * rows), left(1, 2 * rows)], axis=0),
                wide[which, p], preferred_element_type=jnp.float32,
            )
            rest = jnp.dot(
                jnp.concatenate([left(0, rows), left(1, rows)], axis=0),
                fix[which, p], preferred_element_type=jnp.float32,
            )
            for i in range(2):
                cols = slice(i * blk, (i + 1) * blk)
                total = (
                    main[2 * i * rows : (2 * i + 1) * rows, cols]
                    + rest[i * rows : (i + 1) * rows, cols]
                    + main[(2 * i + 1) * rows : (2 * i + 2) * rows, cols]
                )
                emit(z + i, newton(total * (1.0 / LIFT), delta_t))

    def prepare(which):
        @pl.loop(0, pieces)
        def _(c):
            load(which, c).wait()
            if which == 0:

                @pl.when(c == pieces - 1)
                def _():
                    for later in range(pieces):
                        load(1, later).start()

            for zz in range(part):
                z = c * part + zz
                p = c * (part // 2) + zz // 2
                cols = slice((zz % 2) * blk, (zz % 2 + 1) * blk)
                for k in range(3):
                    turned = raw[which, z, k].T * LIFT
                    high = turned.astype(jnp.bfloat16)
                    wide[which, p, k * blk : (k + 1) * blk, cols] = high
                    fix[which, p, k * blk : (k + 1) * blk, cols] = (turned - high.astype(jnp.float32)).astype(F8)

    def fine_step(t, src, sink, keep=True, turn=0):
        def emit(z, s):
            value = s + forcing_at(t, z)
            if keep:
                put(1 - src, z, value)
            sink(z, value)

        propagate(src, 0, DELTA, emit, turn)

    def store_to(buf):
        def emit(z, value):
            buf[z] = value

        return emit

    def drop(z, value):
        pass

    prepare(0)
    for copy in state_loads:
        copy.wait()

    @pl.when(me == 0)
    def _():
        for z in range(zones):
            put(0, z, initial_at(z))
        fine_step(0, 0, drop)

    @pl.when(me > 0)
    def _():
        for z in range(zones):
            put(1, z, forcing_at(0, z))

    for t in range(1, M):
        fine_step(t, t % 2, store_to(ubuf) if t == M - 1 else drop, keep=t < M - 1, turn=t)
    pl.semaphore_wait(barrier, n - 1)

    onward = pltpu.make_async_remote_copy(
        src_ref=ubuf, dst_ref=carr, send_sem=carr_send, recv_sem=carr_recv,
        device_id={"tm": lax.rem(me + 1, n)}, device_id_type=MESH,
    )

    @pl.when(me < n - 1)
    def _():
        onward.start()

    prepare(1)

    @pl.when(me == 0)
    def _():
        for z in range(zones):
            rbuf[0, z] = ubuf[z]
            pbuf[z] = initial_at(z)

    @pl.when(me > 0)
    def _():
        onward.wait_recv()

    @pl.when(me == 1)
    def _():
        for z in range(zones):
            put(0, z, carr[z])
            pbuf[z] = jnp.zeros((rows, blk), jnp.float32)

    @pl.when(me > 1)
    def _():
        for z in range(zones):
            put(0, z, carr[z])
        propagate(0, 1, coarse_dt, store_to(pbuf))

    @pl.when(me > 0)
    def _():
        for t in range(M - 1):
            fine_step(t, t % 2, drop, turn=t)

        def right_side(z, value):
            rbuf[me, z] = value - pbuf[z]

        fine_step(M - 1, (M - 1) % 2, right_side, keep=False, turn=M - 1)

    def share(target):
        return pltpu.make_async_remote_copy(
            src_ref=rbuf.at[me], dst_ref=rbuf.at[me], send_sem=r_send.at[target], recv_sem=r_recv.at[me],
            device_id={"tm": target}, device_id_type=MESH,
        )

    def forward(j):
        return pltpu.make_async_remote_copy(
            src_ref=rbuf.at[j], dst_ref=rbuf.at[j], send_sem=fwd_send.at[j], recv_sem=r_recv.at[j],
            device_id={"tm": lax.rem(me + n - 1, n)}, device_id_type=MESH,
        )

    def sends(target):
        return jnp.logical_and(me > 0, me < target)

    for target in range(n - 1, 1, -2):

        @pl.when(sends(target))
        def _():
            share(target).start()

    def arrive(j):
        forward(j).wait_recv()

        @pl.when(jnp.logical_and(odd == 1, j < me - 1))
        def _():
            forward(j).start()

    @pl.when(me == 0)
    def _():
        for z in range(zones):
            put(0, z, pbuf[z])

    @pl.when(me == 1)
    def _():
        for z in range(zones):
            put(0, z, carr[z])

    @pl.when(me > 1)
    def _():
        arrive(1)
        for z in range(zones):
            put(0, z, rbuf[1, z])

    def chain(j, _):
        propagate(0, 1, coarse_dt, store_to(pbuf))
        arrive(j)
        for z in range(zones):
            put(0, z, pbuf[z] + rbuf[j, z])
        return 0

    lax.fori_loop(2, me, chain, 0)

    def corner(z, value):
        emit_out(M - 1, z, jnp.where(me > 1, value, 0.0) + rbuf[me, z])

    propagate(0, 1, coarse_dt, corner)
    for t in range(M - 1):
        fine_step(t, t % 2, functools.partial(emit_out, t), keep=t < M - 2, turn=t)

    @pl.when(me < n - 1)
    def _():
        onward.wait_send()

    for target in range(n - 1, 1, -2):

        @pl.when(sends(target))
        def _():
            share(target).wait_send()

    def drain(j, _):
        forward(j).wait_send()
        return 0

    lax.fori_loop(1, jnp.where(odd == 1, me - 1, 1), drain, 0)


def solution(mesh):
    n = mesh.shape["tm"]

    def body(initial, forcing, fine_blocks, coarse_blocks):
        inst, slots, cells = forcing.shape
        zones, _, blk, _ = fine_blocks.shape
        blocks = cells // blk
        reps = blocks // zones
        rows = inst * reps
        assert slots == M and n % 2 == 0 and zones % 2 == 0
        pieces = 4 if zones % 4 == 0 else 1
        init_rows = initial.reshape(inst, blocks, blk).transpose(1, 0, 2).reshape(-1, blk)
        forc_rows = forcing.reshape(inst, slots, blocks, blk).transpose(0, 2, 1, 3).reshape(-1, blk)
        state = pltpu.VMEM((zones, rows, blk), jnp.float32)
        out = pl.pallas_call(
            functools.partial(kernel, n, inst, zones, reps, pieces),
            out_shape=pltpu.VMEM(forc_rows.shape, jnp.float32),
            in_specs=[pl.BlockSpec(memory_space=pltpu.HBM)] * 4,
            out_specs=pl.BlockSpec(memory_space=pltpu.VMEM),
            scratch_shapes=[
                pltpu.VMEM(init_rows.shape, jnp.float32),
                pltpu.VMEM(forc_rows.shape, jnp.float32),
                pltpu.VMEM((2,) + fine_blocks.shape, jnp.float32),
                pltpu.VMEM((2, zones // 2, 3 * blk, 2 * blk), jnp.bfloat16),
                pltpu.VMEM((2, zones // 2, 3 * blk, 2 * blk), F8),
                pltpu.VMEM((2, zones + 2, 2 * rows, blk), jnp.bfloat16),
                state,
                state,
                pltpu.VMEM((n, zones, rows, blk), jnp.float32),
                state,
                pltpu.SemaphoreType.DMA((2, pieces)),
                pltpu.SemaphoreType.DMA((2,)),
                pltpu.SemaphoreType.DMA,
                pltpu.SemaphoreType.DMA,
                pltpu.SemaphoreType.DMA((n,)),
                pltpu.SemaphoreType.DMA((n,)),
                pltpu.SemaphoreType.DMA((n,)),
            ],
            compiler_params=pltpu.CompilerParams(collective_id=0, has_side_effects=True),
        )(init_rows, forc_rows, fine_blocks, coarse_blocks)
        return out.reshape(inst, blocks, slots, blk).transpose(0, 2, 1, 3).reshape(forcing.shape)

    in_specs = (P("grp", None), P("grp", "tm", None), P(), P())
    out_specs = P("grp", "tm", None)
    return jax.shard_map(body, mesh=mesh, in_specs=in_specs, out_specs=out_specs, check_vma=False)
```

```python
import functools

import jax
import jax.numpy as jnp
from jax import lax
from jax.experimental import pallas as pl
from jax.experimental.pallas import tpu as pltpu
from jax.sharding import PartitionSpec as P

M = 4
DELTA = 0.05
MESH = pl.DeviceIdType.MESH
F8 = jnp.float8_e4m3fn


def newton(mixing, delta_t):
    solved = mixing
    for _ in range(2):
        squared = solved * solved
        solved = (mixing + (2.0 * delta_t) * solved * squared) / (
            (1.0 - delta_t) + (3.0 * delta_t) * squared
        )
    return solved


LIFTS = (2.0**8, 1.0, 2.0**10)


def kernel(
    n, inst, zones, reps, pieces,
    init_hbm, forc_hbm, fine_hbm, coarse_hbm, out_ref,
    init_ref, forc_ref, next_ref, raw, upper, lower, x, ubuf, carr, rbuf, pbuf,
    load_sem, state_sem, next_send, next_recv, carr_send, carr_recv, r_send, r_recv, fwd_send,
):
    me = lax.axis_index("tm")
    blk = raw.shape[-1]
    rows = inst * reps
    coarse_dt = DELTA * M
    part = zones // pieces
    pairs = zones // 2
    odd = lax.rem(me, 2)

    def load(which, c):
        span = pl.ds(c * part, part)
        return pltpu.make_async_copy((fine_hbm, coarse_hbm)[which].at[span], raw.at[which, span], load_sem.at[which, c])

    state_loads = [
        pltpu.make_async_copy(init_hbm, init_ref, state_sem.at[0]),
        pltpu.make_async_copy(forc_hbm, forc_ref, state_sem.at[1]),
    ]
    load(0, 0).start()
    for copy in state_loads:
        copy.start()
    for c in range(1, pieces):
        load(0, c).start()

    barrier = pltpu.get_barrier_semaphore()
    for step in range(1, n):
        pl.semaphore_signal(barrier, inc=1, device_id={"tm": lax.rem(me + step, n)}, device_id_type=MESH)

    def initial_at(z):
        return jnp.concatenate(
            [init_ref[pl.ds(z * inst + i, reps, stride=zones * inst), :] for i in range(inst)], axis=0
        )

    def forcing_at(ref, slot, z):
        return jnp.concatenate(
            [ref[pl.ds((i * reps * zones + z) * M + slot, reps, stride=zones * M), :] for i in range(inst)],
            axis=0,
        )

    def emit_out(slot, z, value):
        for i in range(inst):
            out_ref[pl.ds((i * reps * zones + z) * M + slot, reps, stride=zones * M), :] = value[
                i * reps : (i + 1) * reps
            ]

    row = lax.broadcasted_iota(jnp.int32, (rows, blk), 0)

    def put(dst, z, value):
        def write(slot, v):
            high = v.astype(jnp.bfloat16)
            low = (v - high.astype(jnp.float32)).astype(jnp.bfloat16)
            x[dst, slot, :rows] = high
            x[dst, slot, rows:] = low

        write(z + 1, value)
        if z == 0:
            rolled = pltpu.roll(value, rows - 1, 0)
            write(zones + 1, jnp.where(row % reps == reps - 1, 0.0, rolled))
        if z == zones - 1:
            rolled = pltpu.roll(value, 1, 0)
            write(0, jnp.where(row % reps == 0, 0.0, rolled))

    def propagate(src, which, delta_t, emit, turn=0, span=None):
        for q in span or range(pairs):
            p = (q + turn) % pairs
            z = 2 * p

            def left(i, stop):
                return jnp.concatenate([x[src, z + i + k, :stop] for k in range(3)], axis=1)

            tail = jnp.dot(
                jnp.concatenate([left(0, rows), left(1, rows)], axis=0),
                lower[which, p], preferred_element_type=jnp.float32,
            )
            for i in range(2):
                acc = jnp.dot(left(i, 2 * rows), upper[which, z + i], preferred_element_type=jnp.float32)
                cols = slice(i * blk, (i + 1) * blk)
                second = acc[:rows, blk:] + acc[rows:, blk:] + tail[i * rows : (i + 1) * rows, cols] * (1.0 / LIFTS[2])
                total = acc[:rows, :blk] + acc[rows:, :blk] + second
                emit(z + i, newton(total * (1.0 / LIFTS[0]), delta_t))

    def slices(which, z, p, cols):
        for k in range(3):
            span = slice(k * blk, (k + 1) * blk)
            rest = raw[which, z, k].T
            for s, lift in enumerate(LIFTS):
                if lift != 1.0:
                    rest = rest * lift
                piece = rest.astype(F8)
                if s < 2:
                    upper[which, z, span, s * blk : (s + 1) * blk] = piece
                    rest = rest - piece.astype(jnp.float32)
                else:
                    lower[which, p, span, cols] = piece

    def columns(zz):
        return slice((zz % 2) * blk, (zz % 2 + 1) * blk)

    def prepare_coarse():
        @pl.loop(0, pieces)
        def _(c):
            load(1, c).wait()
            for zz in range(part):
                slices(1, c * part + zz, c * (part // 2) + zz // 2, columns(zz))

    def fine_step(t, src, sink, keep=True, turn=0, forcing=forc_ref, span=None):
        def emit(z, s):
            value = s + forcing_at(forcing, t, z)
            if keep:
                put(1 - src, z, value)
            sink(z, value)

        propagate(src, 0, DELTA, emit, turn, span)

    def store_to(buf):
        def emit(z, value):
            buf[z] = value

        return emit

    def drop(z, value):
        pass

    partner = me + 1 - 2 * odd
    swap = pltpu.make_async_remote_copy(
        src_ref=forc_ref, dst_ref=next_ref, send_sem=next_send, recv_sem=next_recv,
        device_id={"tm": partner}, device_id_type=MESH,
    )
    middle = pieces // 2

    def open_up(t, src, start):
        half = part // 2
        for c in range(pieces):
            load(0, c).wait()
            if c == pieces - 1:
                for later in range(pieces):
                    load(1, later).start()
            if c == middle:
                for copy in state_loads:
                    copy.wait()
            for zz in range(part):
                z = c * part + zz
                slices(0, z, z // 2, columns(zz))
            if c == middle:
                for z in range(zones):
                    put(src, z, start(z))
            if c > middle:
                fine_step(t, src, drop, span=range(0 if c == middle + 1 else (c - 1) * half, c * half))
        fine_step(t, src, drop, span=range((pieces - 1) * half if pieces > 2 else 0, pairs))
        pl.semaphore_wait(barrier, n - 1)
        swap.start()

    @pl.when(me == 0)
    def _():
        open_up(0, 0, initial_at)
        fine_step(1, 1, drop, turn=1)
        fine_step(2, 0, drop, turn=2)
        fine_step(3, 1, store_to(ubuf), turn=3)

    @pl.when(me > 0)
    def _():
        open_up(1, 1, functools.partial(forcing_at, forc_ref, 0))
        for t in range(2, M):
            fine_step(t, t % 2, store_to(ubuf) if t == M - 1 else drop, keep=t < M - 1, turn=t - 1)

    onward = pltpu.make_async_remote_copy(
        src_ref=ubuf, dst_ref=carr, send_sem=carr_send, recv_sem=carr_recv,
        device_id={"tm": jnp.where(me == 0, 1, lax.rem(me + 2, n))}, device_id_type=MESH,
    )
    hands_on = jnp.logical_or(me == 0, jnp.logical_and(odd == 1, me < n - 2))

    @pl.when(jnp.logical_and(hands_on, me > 0))
    def _():
        onward.start()

    def interval(sink, beside=None, turn=0):
        for t in range(M):
            fine_step(
                t, t % 2, sink if t == M - 1 else drop, keep=t < M - 1, turn=turn + max(t - 1, 0), forcing=next_ref
            )
            if t == 0 and beside is not None:
                beside()

    def share(target, j):
        return pltpu.make_async_remote_copy(
            src_ref=rbuf.at[j], dst_ref=rbuf.at[j], send_sem=r_send.at[target], recv_sem=r_recv.at[j],
            device_id={"tm": target}, device_id_type=MESH,
        )

    def forward(j):
        return pltpu.make_async_remote_copy(
            src_ref=rbuf.at[j], dst_ref=rbuf.at[j], send_sem=fwd_send.at[j], recv_sem=r_recv.at[j],
            device_id={"tm": lax.rem(me + n - 1, n)}, device_id_type=MESH,
        )

    first_targets = (3, 1)
    far_targets = range(n - 1, 2, -2)

    def each_share(act):
        for target in far_targets:

            @pl.when(jnp.logical_and(me > 1, me < target))
            def _():
                act(share(target, partner))

        @pl.when(jnp.logical_and(odd == 1, me > 1))
        def _():
            act(share(partner, partner))

    @pl.when(me == 0)
    def _():
        swap.wait_recv()
        interval(store_to(rbuf.at[1]), turn=4)
        onward.start()
        for target in first_targets:
            share(target, 1).start()
        for z in range(zones):
            rbuf[0, z] = ubuf[z]

    prepare_coarse()

    @pl.when(jnp.logical_and(odd == 0, me > 0))
    def _():
        for z in range(zones):
            put(0, z, ubuf[z])
        swap.wait_recv()

    @pl.when(odd == 1)
    def _():
        onward.wait_recv()
        for z in range(zones):
            put(0, z, carr[z])
        swap.wait_recv()

    @pl.when(me > 1)
    def _():
        def right_side(z, value):
            rbuf[partner, z] = value - pbuf[z]

        interval(right_side, lambda: propagate(0, 1, coarse_dt, store_to(pbuf)))

    @pl.when(me == 3)
    def _():
        forward(1).wait_recv()
        forward(1).start()
        for z in range(zones):
            put(0, z, rbuf[1, z])

        def second(z, value):
            rbuf[2, z] = value + rbuf[2, z]

        propagate(0, 1, coarse_dt, second)

    each_share(lambda copy: copy.start())

    def arrive(j):
        forward(j).wait_recv()

        @pl.when(jnp.logical_and(odd == 1, j < me - 1))
        def _():
            forward(j).start()

    @pl.when(me == 0)
    def _():
        for z in range(zones):
            put(0, z, initial_at(z))

    @pl.when(me == 1)
    def _():
        for z in range(zones):
            put(0, z, carr[z])

    @pl.when(me == 2)
    def _():
        forward(1).wait_recv()
        for z in range(zones):
            put(0, z, rbuf[1, z])

    @pl.when(me > 3)
    def _():
        arrive(2)

    @pl.when(me > 2)
    def _():
        first = lax.rem(me + 1, 2)
        for z in range(zones):
            put(first, z, rbuf[2, z])

    def reach(left_over):
        j = me - 1 - left_over
        if left_over > 0:
            arrive(j)
        else:

            @pl.when(odd == 0)
            def _():
                arrive(j)

    def chain(left_over, turn=0):
        def emit(z, value):
            put(left_over % 2, z, value + rbuf[me - 1 - left_over, z])

        propagate((left_over + 1) % 2, 1, coarse_dt, emit, turn)

    for left_over in range(n - 5, -1, -1):
        if left_over % 2 == 0:

            @pl.when(me == left_over + 4)
            def _():
                reach(left_over)
                chain(left_over)

        else:

            @pl.when(me > left_over + 3)
            def _():
                reach(left_over)
                reach(left_over - 1)
                chain(left_over)
                chain(left_over - 1, 1)

    @pl.when(me > 0)
    def _():
        forward(me).wait_recv()

    def corner(z, value):
        emit_out(M - 1, z, jnp.where(me > 2, value, 0.0) + rbuf[me, z])

    for t in range(M - 1):
        fine_step(t, t % 2, functools.partial(emit_out, t), keep=t < M - 2, turn=max(t - 1, 0))
        if t == 0:
            propagate(0, 1, coarse_dt, corner)

    swap.wait_send()

    @pl.when(hands_on)
    def _():
        onward.wait_send()

    @pl.when(me == 0)
    def _():
        for target in first_targets:
            share(target, 1).wait_send()

    each_share(lambda copy: copy.wait_send())

    def drain(j, _):
        forward(j).wait_send()
        return 0

    lax.fori_loop(jnp.where(me == 3, 1, 2), jnp.where(odd == 1, me - 1, 2), drain, 0)


def solution(mesh):
    n = mesh.shape["tm"]

    def body(initial, forcing, fine_blocks, coarse_blocks):
        inst, slots, cells = forcing.shape
        zones, _, blk, _ = fine_blocks.shape
        blocks = cells // blk
        reps = blocks // zones
        rows = inst * reps
        assert slots == M and n > 4 and n % 2 == 0 and zones % 2 == 0
        pieces = 4 if zones % 4 == 0 else 1
        init_rows = initial.reshape(inst, blocks, blk).transpose(1, 0, 2).reshape(-1, blk)
        forc_rows = forcing.reshape(inst, slots, blocks, blk).transpose(0, 2, 1, 3).reshape(-1, blk)
        state = pltpu.VMEM((zones, rows, blk), jnp.float32)
        out = pl.pallas_call(
            functools.partial(kernel, n, inst, zones, reps, pieces),
            out_shape=pltpu.VMEM(forc_rows.shape, jnp.float32),
            in_specs=[pl.BlockSpec(memory_space=pltpu.HBM)] * 4,
            out_specs=pl.BlockSpec(memory_space=pltpu.VMEM),
            scratch_shapes=[
                pltpu.VMEM(init_rows.shape, jnp.float32),
                pltpu.VMEM(forc_rows.shape, jnp.float32),
                pltpu.VMEM(forc_rows.shape, jnp.float32),
                pltpu.VMEM((2,) + fine_blocks.shape, jnp.float32),
                pltpu.VMEM((2, zones, 3 * blk, 2 * blk), F8),
                pltpu.VMEM((2, zones // 2, 3 * blk, 2 * blk), F8),
                pltpu.VMEM((2, zones + 2, 2 * rows, blk), jnp.bfloat16),
                state,
                state,
                pltpu.VMEM((n, zones, rows, blk), jnp.float32),
                state,
                pltpu.SemaphoreType.DMA((2, pieces)),
                pltpu.SemaphoreType.DMA((2,)),
                pltpu.SemaphoreType.DMA,
                pltpu.SemaphoreType.DMA,
                pltpu.SemaphoreType.DMA,
                pltpu.SemaphoreType.DMA,
                pltpu.SemaphoreType.DMA((n,)),
                pltpu.SemaphoreType.DMA((n,)),
                pltpu.SemaphoreType.DMA((n,)),
            ],
            compiler_params=pltpu.CompilerParams(collective_id=0, has_side_effects=True),
        )(init_rows, forc_rows, fine_blocks, coarse_blocks)
        return out.reshape(inst, blocks, slots, blk).transpose(0, 2, 1, 3).reshape(forcing.shape)

    in_specs = (P("grp", None), P("grp", "tm", None), P(), P())
    out_specs = P("grp", "tm", None)
    return jax.shard_map(body, mesh=mesh, in_specs=in_specs, out_specs=out_specs, check_vma=False)
```

```python
import functools

import jax
import jax.numpy as jnp
from jax import lax
from jax.experimental import pallas as pl
from jax.experimental.pallas import tpu as pltpu
from jax.sharding import PartitionSpec as P

M = 4
DELTA = 0.05
MESH = pl.DeviceIdType.MESH
F8 = jnp.float8_e4m3fn


def newton(mixing, delta_t):
    solved = mixing
    for _ in range(2):
        squared = solved * solved
        solved = (mixing + (2.0 * delta_t) * solved * squared) / (
            (1.0 - delta_t) + (3.0 * delta_t) * squared
        )
    return solved


LIFTS = (2.0**8, 1.0, 2.0**10)
HALVES = 2


def kernel(
    n, inst, zones, reps, pieces,
    init_hbm, forc_hbm, fine_hbm, coarse_hbm, out_ref,
    init_ref, forc_ref, next_ref, raw, upper, lower, x, start_x, ubuf, carr, rbuf, pbuf,
    load_sem, state_sem, next_send, next_recv, carr_send, carr_recv, r_send, r_recv, fwd_send,
):
    me = lax.axis_index("tm")
    blk = raw.shape[-1]
    rows = inst * reps
    coarse_dt = DELTA * M
    part = zones // pieces
    pairs = zones // 2
    odd = lax.rem(me, 2)

    eighth = zones // 8
    fine_cuts = [e * eighth for e in (0, 1, 3, 5, 7, 8)] if eighth > 1 and eighth % 2 == 0 else [0, zones]
    blocks = len(fine_cuts) - 1

    def load(c):
        span = pl.ds(fine_cuts[c], fine_cuts[c + 1] - fine_cuts[c])
        return pltpu.make_async_copy(fine_hbm.at[span], raw.at[0, span], load_sem.at[c])

    coarse_load = pltpu.make_async_copy(coarse_hbm, raw.at[1], load_sem.at[blocks])

    state_loads = [
        pltpu.make_async_copy(init_hbm, init_ref, state_sem.at[0]),
        pltpu.make_async_copy(forc_hbm, forc_ref, state_sem.at[1]),
    ]
    state_loads[0].start()
    load(0).start()
    state_loads[1].start()
    for c in range(1, blocks):
        load(c).start()

    barrier = pltpu.get_barrier_semaphore()
    for step in range(1, n):
        pl.semaphore_signal(barrier, inc=1, device_id={"tm": lax.rem(me + step, n)}, device_id_type=MESH)

    def initial_at(z):
        return jnp.concatenate(
            [init_ref[pl.ds(z * inst + i, reps, stride=zones * inst), :] for i in range(inst)], axis=0
        )

    def forcing_at(ref, slot, z):
        return jnp.concatenate(
            [ref[pl.ds((i * reps * zones + z) * M + slot, reps, stride=zones * M), :] for i in range(inst)],
            axis=0,
        )

    def emit_out(slot, z, value):
        for i in range(inst):
            out_ref[pl.ds((i * reps * zones + z) * M + slot, reps, stride=zones * M), :] = value[
                i * reps : (i + 1) * reps
            ]

    row = lax.broadcasted_iota(jnp.int32, (rows, blk), 0)

    def state_of(where):
        return x.at[where] if isinstance(where, int) else where

    def put(dst, z, value):
        held = state_of(dst)

        def write(slot, v):
            high = v.astype(jnp.bfloat16)
            low = (v - high.astype(jnp.float32)).astype(jnp.bfloat16)
            held[slot, :rows] = high
            held[slot, rows:] = low

        write(z + 1, value)
        if z == 0:
            rolled = pltpu.roll(value, rows - 1, 0)
            write(zones + 1, jnp.where(row % reps == reps - 1, 0.0, rolled))
        if z == zones - 1:
            rolled = pltpu.roll(value, 1, 0)
            write(0, jnp.where(row % reps == 0, 0.0, rolled))

    def propagate(src, which, delta_t, emit, turn=0, span=None):
        held = state_of(src)
        for q in range(pairs) if span is None else span:
            p = (q + turn) % pairs
            z = 2 * p

            def left(i, stop):
                return jnp.concatenate([held[z + i + k, :stop] for k in range(3)], axis=1)

            tail = jnp.dot(
                jnp.concatenate([left(0, rows), left(1, rows)], axis=0),
                lower[which, p], preferred_element_type=jnp.float32,
            )
            for i in range(2):
                acc = jnp.dot(left(i, 2 * rows), upper[which, z + i], preferred_element_type=jnp.float32)
                cols = slice(i * blk, (i + 1) * blk)
                second = acc[:rows, blk:] + acc[rows:, blk:] + tail[i * rows : (i + 1) * rows, cols] * (1.0 / LIFTS[2])
                total = acc[:rows, :blk] + acc[rows:, :blk] + second
                emit(z + i, newton(total * (1.0 / LIFTS[0]), delta_t))

    def slices(which, z, p, cols):
        for k in range(3):
            span = slice(k * blk, (k + 1) * blk)
            rest = raw[which, z, k].T
            for s, lift in enumerate(LIFTS):
                if lift != 1.0:
                    rest = rest * lift
                piece = rest.astype(F8)
                if s < 2:
                    upper[which, z, span, s * blk : (s + 1) * blk] = piece
                    rest = rest - piece.astype(jnp.float32)
                else:
                    lower[which, p, span, cols] = piece

    def columns(zz):
        return slice((zz % 2) * blk, (zz % 2 + 1) * blk)

    def prepare_coarse():
        coarse_load.wait()

        @pl.loop(0, pieces)
        def _(c):
            for zz in range(part):
                slices(1, c * part + zz, c * (part // 2) + zz // 2, columns(zz))

    def fine_step(t, src, sink, keep=True, turn=0, forcing=forc_ref, span=None):
        def emit(z, s):
            value = s + forcing_at(forcing, t, z)
            if keep:
                put(1 - src, z, value)
            sink(z, value)

        propagate(src, 0, DELTA, emit, turn, span)

    def store_to(buf):
        def emit(z, value):
            buf[z] = value

        return emit

    def drop(z, value):
        pass

    partner = me + 1 - 2 * odd
    half = zones // HALVES
    parts_of = [range(h * (pairs // HALVES), (h + 1) * (pairs // HALVES)) for h in range(HALVES)]
    swap = pltpu.make_async_remote_copy(
        src_ref=forc_ref, dst_ref=next_ref, send_sem=next_send, recv_sem=next_recv,
        device_id={"tm": partner}, device_id_type=MESH,
    )

    def open_up(t, src, start):
        state_at = max(blocks - 2, 0)
        done = 0
        for c in range(blocks):
            load(c).wait()
            if c == state_at:
                coarse_load.start()
                for copy in state_loads:
                    copy.wait()
                for z in range(zones):
                    put(src, z, start(z))
            if c >= state_at:
                fine_step(t, src, drop, span=range(done, fine_cuts[c] // 2))
                done = fine_cuts[c] // 2
            for z in range(fine_cuts[c], fine_cuts[c + 1]):
                slices(0, z, z // 2, columns(z))
        fine_step(t, src, drop, span=range(done, pairs))
        pl.semaphore_wait(barrier, n - 1)
        swap.start()

    @pl.when(me == 0)
    def _():
        open_up(0, 0, initial_at)
        fine_step(1, 1, drop, turn=1)
        fine_step(2, 0, drop, turn=2)
        fine_step(3, 1, store_to(ubuf), turn=3)

    def onward(h):
        span = pl.ds(h * half, half)
        return pltpu.make_async_remote_copy(
            src_ref=ubuf.at[span], dst_ref=carr.at[span], send_sem=carr_send.at[h], recv_sem=carr_recv.at[h],
            device_id={"tm": jnp.where(me == 0, 1, lax.rem(me + 2, n))}, device_id_type=MESH,
        )

    hands_on = jnp.logical_and(odd == 1, me < n - 2)

    @pl.when(me > 0)
    def _():
        open_up(1, 1, functools.partial(forcing_at, forc_ref, 0))
        for t in range(2, M - 1):
            fine_step(t, t % 2, drop, turn=t + 1)
        for h in (1, 0):
            fine_step(M - 1, (M - 1) % 2, store_to(ubuf), keep=False, turn=pairs // 2, span=parts_of[1 - h])

            @pl.when(hands_on)
            def _():
                onward(h).start()

    def interval(sink, beside=None, turn=0, mid=None):
        for t in range(M):
            args = dict(keep=t < M - 1, turn=turn + t + (beside is not None and t > 0), forcing=next_ref)
            if t < M - 1:
                fine_step(t, t % 2, drop, **args)
            else:
                for h in range(HALVES):
                    fine_step(t, t % 2, sink, span=parts_of[h], **args)
                    if mid is not None:
                        mid(h)
            if t == 0 and beside is not None:
                beside()

    def message(j, h):
        return rbuf.at[j, pl.ds(h * half, half)] if h is not None else rbuf.at[j]

    def landed(j, h):
        return r_recv.at[j if not h else n + j - 1]

    def share(target, j, h):
        return pltpu.make_async_remote_copy(
            src_ref=message(j, h), dst_ref=message(j, h), send_sem=r_send.at[target // 2, h or 0],
            recv_sem=landed(j, h), device_id={"tm": target}, device_id_type=MESH,
        )

    def forward(j, h):
        return pltpu.make_async_remote_copy(
            src_ref=message(j, h), dst_ref=message(j, h), send_sem=fwd_send.at[j if not h else 0],
            recv_sem=landed(j, h), device_id={"tm": lax.rem(me + n - 1, n)}, device_id_type=MESH,
        )

    first_targets = (3, 1)
    far_targets = range(3, n, 2)

    def each_share(act, h):
        for target in far_targets:

            @pl.when(jnp.logical_and(me > 1, me < target))
            def _():
                act(share(target, partner, h))

        @pl.when(jnp.logical_and(odd == 1, me > 1))
        def _():
            act(share(partner, partner, h))

    def start(copy):
        copy.start()

    def wait_send(copy):
        copy.wait_send()

    @pl.when(me == 0)
    def _():
        swap.wait_recv()

        def first_share(h):
            for target in first_targets:
                share(target, 1, h).start()

        interval(store_to(rbuf.at[1]), turn=M + 1, mid=first_share)
        for h in range(HALVES):
            onward(h).start()
        for z in range(zones):
            rbuf[0, z] = ubuf[z]

    prepare_coarse()

    @pl.when(jnp.logical_and(odd == 0, me > 0))
    def _():
        for z in range(zones):
            put(0, z, ubuf[z])
        swap.wait_recv()

    @pl.when(odd == 1)
    def _():
        for h in (1, 0):
            onward(h).wait_recv()
            for z in range(h * half, (h + 1) * half):
                put(0, z, carr[z])
        swap.wait_recv()

    @pl.when(me > 1)
    def _():
        def right_side(z, value):
            rbuf[partner, z] = value - pbuf[z]

        interval(right_side, lambda: propagate(0, 1, coarse_dt, store_to(pbuf)))

    early = list(range(1, parts_of[0].stop - 1))
    late = [p for p in range(pairs) if p not in early]
    late = [[p for p in late if p in parts_of[0]], [p for p in late if p not in parts_of[0]]]

    @pl.when(me == 3)
    def _():
        def second(z, value):
            rbuf[2, z] = value + rbuf[2, z]

        for h in range(HALVES):
            forward(1, h).wait_recv()
            for z in range(h * half, (h + 1) * half):
                put(0, z, rbuf[1, z])
            if h == 0:
                propagate(0, 1, coarse_dt, second, span=early)
        forward(1, None).start()
        for h in range(HALVES):
            propagate(0, 1, coarse_dt, second, span=late[h])
            each_share(start, h)

    @pl.when(me != 3)
    def _():
        each_share(start, None)

    def arrive(j, h=None):
        forward(j, h).wait_recv()

        @pl.when(jnp.logical_and(odd == 1, j < me - 1))
        def _():
            forward(j, h).start()

    @pl.when(me == 0)
    def _():
        for z in range(zones):
            put(0, z, initial_at(z))

    @pl.when(me == 1)
    def _():
        for z in range(zones):
            put(0, z, carr[z])

    @pl.when(me == 2)
    def _():
        forward(1, None).wait_recv()
        for z in range(zones):
            put(0, z, rbuf[1, z])

    for j in range(3, n - 1, 2):

        @pl.when(me > j)
        def _():
            arrive(j)

    @pl.when(me == 3)
    def _():
        for z in range(zones):
            put(0, z, rbuf[2, z])

    def chain(src, dst, j, span=None, turn=0):
        def emit(z, value):
            put(dst, z, value + rbuf[j, z])

        propagate(src, 1, coarse_dt, emit, turn, span)

    def begin(parity):
        for h in range(HALVES):
            arrive(2, h)
            for z in range(h * half, (h + 1) * half):
                put(start_x, z, rbuf[2, z])
            if h == 0:
                chain(start_x, parity, 3, early)
        if parity == 1:

            @pl.when(me > 5)
            def _():
                arrive(4)

        chain(start_x, parity, 3, late[0][1:] + late[1] + late[0][:1])
        if parity == 1:
            chain(1, 0, 4, turn=late[0][-1] + 1)

    for parity in range(2):

        @pl.when(jnp.logical_and(me > 3, odd == parity))
        def _():
            begin(parity)

    for left_over in range(n - 5 - n % 2, 0, -1):
        if left_over % 2 == 1:

            @pl.when(me > left_over + 4)
            def _():
                j = me - 1 - left_over

                @pl.when(jnp.logical_or(odd == 0, left_over > 1))
                def _():
                    arrive(j + odd)

                chain(0, 1, j)
                chain(1, 0, j + 1, turn=1)

    @pl.when(jnp.logical_or(me == 1, me == 2))
    def _():
        for h in range(HALVES):
            forward(me, h).wait_recv()

    @pl.when(me > 2)
    def _():
        forward(me, None).wait_recv()

    def corner(z, value):
        emit_out(M - 1, z, jnp.where(me > 2, value, 0.0) + rbuf[me, z])

    for t in range(M - 1):
        fine_step(t, t % 2, functools.partial(emit_out, t), keep=t < M - 2, turn=max(t - 1, 0))
        if t == 0:
            propagate(0, 1, coarse_dt, corner)

    swap.wait_send()
    for h in range(HALVES):

        @pl.when(jnp.logical_or(hands_on, me == 0))
        def _():
            onward(h).wait_send()

        @pl.when(me == 0)
        def _():
            for target in first_targets:
                share(target, 1, h).wait_send()

        @pl.when(me == 3)
        def _():
            each_share(wait_send, h)

    @pl.when(me != 3)
    def _():
        each_share(wait_send, None)

    @pl.when(me == 3)
    def _():
        forward(1, None).wait_send()

    @pl.when(jnp.logical_and(odd == 1, me > 3))
    def _():
        for h in range(HALVES):
            forward(2, h).wait_send()

    def drain(j, _):
        forward(j, None).wait_send()
        return 0

    lax.fori_loop(3, jnp.where(odd == 1, me - 1, 3), drain, 0)


def solution(mesh):
    n = mesh.shape["tm"]

    def body(initial, forcing, fine_blocks, coarse_blocks):
        inst, slots, cells = forcing.shape
        zones, _, blk, _ = fine_blocks.shape
        blocks = cells // blk
        reps = blocks // zones
        rows = inst * reps
        assert slots == M and n > 4 and n % 2 == 0 and zones % (2 * HALVES) == 0
        pieces = 4 if zones % 4 == 0 else 1
        init_rows = initial.reshape(inst, blocks, blk).transpose(1, 0, 2).reshape(-1, blk)
        forc_rows = forcing.reshape(inst, slots, blocks, blk).transpose(0, 2, 1, 3).reshape(-1, blk)
        state = pltpu.VMEM((zones, rows, blk), jnp.float32)
        out = pl.pallas_call(
            functools.partial(kernel, n, inst, zones, reps, pieces),
            out_shape=pltpu.VMEM(forc_rows.shape, jnp.float32),
            in_specs=[pl.BlockSpec(memory_space=pltpu.HBM)] * 4,
            out_specs=pl.BlockSpec(memory_space=pltpu.VMEM),
            scratch_shapes=[
                pltpu.VMEM(init_rows.shape, jnp.float32),
                pltpu.VMEM(forc_rows.shape, jnp.float32),
                pltpu.VMEM(forc_rows.shape, jnp.float32),
                pltpu.VMEM((2,) + fine_blocks.shape, jnp.float32),
                pltpu.VMEM((2, zones, 3 * blk, 2 * blk), F8),
                pltpu.VMEM((2, zones // 2, 3 * blk, 2 * blk), F8),
                pltpu.VMEM((2, zones + 2, 2 * rows, blk), jnp.bfloat16),
                pltpu.VMEM((zones + 2, 2 * rows, blk), jnp.bfloat16),
                state,
                state,
                pltpu.VMEM((n, zones, rows, blk), jnp.float32),
                state,
                pltpu.SemaphoreType.DMA((6,)),
                pltpu.SemaphoreType.DMA((2,)),
                pltpu.SemaphoreType.DMA,
                pltpu.SemaphoreType.DMA,
                pltpu.SemaphoreType.DMA((HALVES,)),
                pltpu.SemaphoreType.DMA((HALVES,)),
                pltpu.SemaphoreType.DMA((n // 2, HALVES)),
                pltpu.SemaphoreType.DMA((n + 2,)),
                pltpu.SemaphoreType.DMA((n - 2,)),
            ],
            compiler_params=pltpu.CompilerParams(collective_id=0, has_side_effects=True),
        )(init_rows, forc_rows, fine_blocks, coarse_blocks)
        return out.reshape(inst, blocks, slots, blk).transpose(0, 2, 1, 3).reshape(forcing.shape)

    in_specs = (P("grp", None), P("grp", "tm", None), P(), P())
    out_specs = P("grp", "tm", None)
    return jax.shard_map(body, mesh=mesh, in_specs=in_specs, out_specs=out_specs, check_vma=False)
```

```python
import functools

import jax
import jax.numpy as jnp
from jax import lax
from jax.experimental import pallas as pl
from jax.experimental.pallas import tpu as pltpu
from jax.sharding import PartitionSpec as P

M = 4
DELTA = 0.05
MESH = pl.DeviceIdType.MESH
F8 = jnp.float8_e4m3fn


def newton(mixing, delta_t):
    solved = mixing
    for _ in range(2):
        squared = solved * solved
        solved = (mixing + (2.0 * delta_t) * solved * squared) / (
            (1.0 - delta_t) + (3.0 * delta_t) * squared
        )
    return solved


LIFTS = (2.0**8, 1.0, 2.0**10)
HALVES = 2


def kernel(
    n, inst, zones, reps, pieces,
    init_hbm, forc_hbm, fine_hbm, coarse_hbm, out_ref,
    init_ref, forc_ref, next_ref, raw, upper, lower, x, start_x, ubuf, carr, rbuf, pbuf,
    load_sem, state_sem, next_send, next_recv, carr_send, carr_recv, r_send, r_recv, fwd_send,
):
    me = lax.axis_index("tm")
    blk = raw.shape[-1]
    rows = inst * reps
    coarse_dt = DELTA * M
    part = zones // pieces
    pairs = zones // 2
    odd = lax.rem(me, 2)

    eighth = zones // 8
    fine_cuts = [e * eighth for e in (0, 1, 3, 5, 7, 8)] if eighth > 1 and eighth % 2 == 0 else [0, zones]
    blocks = len(fine_cuts) - 1

    def load(c):
        span = pl.ds(fine_cuts[c], fine_cuts[c + 1] - fine_cuts[c])
        return pltpu.make_async_copy(fine_hbm.at[span], raw.at[0, span], load_sem.at[c])

    coarse_load = pltpu.make_async_copy(coarse_hbm, raw.at[1], load_sem.at[blocks])

    state_loads = [
        pltpu.make_async_copy(init_hbm, init_ref, state_sem.at[0]),
        pltpu.make_async_copy(forc_hbm, forc_ref, state_sem.at[1]),
    ]
    state_loads[0].start()
    load(0).start()
    state_loads[1].start()
    for c in range(1, blocks):
        load(c).start()

    barrier = pltpu.get_barrier_semaphore()
    for step in range(1, n):
        pl.semaphore_signal(barrier, inc=1, device_id={"tm": lax.rem(me + step, n)}, device_id_type=MESH)

    def initial_at(z):
        return jnp.concatenate(
            [init_ref[pl.ds(z * inst + i, reps, stride=zones * inst), :] for i in range(inst)], axis=0
        )

    def forcing_at(ref, slot, z):
        return jnp.concatenate(
            [ref[pl.ds((i * reps * zones + z) * M + slot, reps, stride=zones * M), :] for i in range(inst)],
            axis=0,
        )

    def emit_out(slot, z, value):
        for i in range(inst):
            out_ref[pl.ds((i * reps * zones + z) * M + slot, reps, stride=zones * M), :] = value[
                i * reps : (i + 1) * reps
            ]

    row = lax.broadcasted_iota(jnp.int32, (rows, blk), 0)

    def state_of(where):
        return x.at[where] if isinstance(where, int) else where

    def put(dst, z, value):
        held = state_of(dst)

        def write(slot, v):
            high = v.astype(jnp.bfloat16)
            low = (v - high.astype(jnp.float32)).astype(jnp.bfloat16)
            held[slot, :rows] = high
            held[slot, rows:] = low

        write(z + 1, value)
        if z == 0:
            rolled = pltpu.roll(value, rows - 1, 0)
            write(zones + 1, jnp.where(row % reps == reps - 1, 0.0, rolled))
        if z == zones - 1:
            rolled = pltpu.roll(value, 1, 0)
            write(0, jnp.where(row % reps == 0, 0.0, rolled))

    def propagate(src, which, delta_t, emit, turn=0, span=None):
        held = state_of(src)
        for q in range(pairs) if span is None else span:
            p = (q + turn) % pairs
            z = 2 * p

            def left(i, stop):
                return jnp.concatenate([held[z + i + k, :stop] for k in range(3)], axis=1)

            tail = jnp.dot(
                jnp.concatenate([left(0, rows), left(1, rows)], axis=0),
                lower[which, p], preferred_element_type=jnp.float32,
            )
            for i in range(2):
                acc = jnp.dot(left(i, 2 * rows), upper[which, z + i], preferred_element_type=jnp.float32)
                cols = slice(i * blk, (i + 1) * blk)
                second = acc[:rows, blk:] + acc[rows:, blk:] + tail[i * rows : (i + 1) * rows, cols] * (1.0 / LIFTS[2])
                total = acc[:rows, :blk] + acc[rows:, :blk] + second
                emit(z + i, newton(total * (1.0 / LIFTS[0]), delta_t))

    def slices(which, z, p, cols):
        for k in range(3):
            span = slice(k * blk, (k + 1) * blk)
            rest = raw[which, z, k].T
            for s, lift in enumerate(LIFTS):
                if lift != 1.0:
                    rest = rest * lift
                piece = rest.astype(F8)
                if s < 2:
                    upper[which, z, span, s * blk : (s + 1) * blk] = piece
                    rest = rest - piece.astype(jnp.float32)
                else:
                    lower[which, p, span, cols] = piece

    def columns(zz):
        return slice((zz % 2) * blk, (zz % 2 + 1) * blk)

    def prepare_coarse():
        coarse_load.wait()

        @pl.loop(0, pieces)
        def _(c):
            for zz in range(part):
                slices(1, c * part + zz, c * (part // 2) + zz // 2, columns(zz))

    def fine_step(t, src, sink, keep=True, turn=0, forcing=forc_ref, span=None):
        def emit(z, s):
            value = s + forcing_at(forcing, t, z)
            if keep:
                put(1 - src, z, value)
            sink(z, value)

        propagate(src, 0, DELTA, emit, turn, span)

    def store_to(buf):
        def emit(z, value):
            buf[z] = value

        return emit

    def drop(z, value):
        pass

    partner = me + 1 - 2 * odd
    half = zones // HALVES
    parts_of = [range(h * (pairs // HALVES), (h + 1) * (pairs // HALVES)) for h in range(HALVES)]
    swap = pltpu.make_async_remote_copy(
        src_ref=forc_ref, dst_ref=next_ref, send_sem=next_send, recv_sem=next_recv,
        device_id={"tm": partner}, device_id_type=MESH,
    )

    def open_up(t, src, start):
        state_at = max(blocks - 2, 0)
        done = 0
        for c in range(blocks):
            load(c).wait()
            if c == state_at:
                coarse_load.start()
                for copy in state_loads:
                    copy.wait()
                for z in range(zones):
                    put(src, z, start(z))
            if c >= state_at:
                fine_step(t, src, drop, span=range(done, fine_cuts[c] // 2))
                done = fine_cuts[c] // 2
            for z in range(fine_cuts[c], fine_cuts[c + 1]):
                slices(0, z, z // 2, columns(z))
        fine_step(t, src, drop, span=range(done, pairs))
        pl.semaphore_wait(barrier, n - 1)
        swap.start()

    @pl.when(me == 0)
    def _():
        open_up(0, 0, initial_at)
        fine_step(1, 1, drop, turn=1)
        fine_step(2, 0, drop, turn=2)
        fine_step(3, 1, store_to(ubuf), turn=3)

    def onward(h):
        span = pl.ds(h * half, half)
        return pltpu.make_async_remote_copy(
            src_ref=ubuf.at[span], dst_ref=carr.at[span], send_sem=carr_send.at[h], recv_sem=carr_recv.at[h],
            device_id={"tm": jnp.where(me == 0, 1, lax.rem(me + 2, n))}, device_id_type=MESH,
        )

    hands_on = jnp.logical_and(odd == 1, me < n - 2)

    @pl.when(me > 0)
    def _():
        open_up(1, 1, functools.partial(forcing_at, forc_ref, 0))
        for t in range(2, M - 1):
            fine_step(t, t % 2, drop, turn=t + 1)
        for h in (1, 0):
            fine_step(M - 1, (M - 1) % 2, store_to(ubuf), keep=False, turn=pairs // 2, span=parts_of[1 - h])

            @pl.when(hands_on)
            def _():
                onward(h).start()

    def interval(sink, beside=None, turn=0, mid=None):
        for t in range(M):
            args = dict(keep=t < M - 1, turn=turn + t + (beside is not None and t > 0), forcing=next_ref)
            if t < M - 1:
                fine_step(t, t % 2, drop, **args)
            else:
                for h in range(HALVES):
                    fine_step(t, t % 2, sink, span=parts_of[h], **args)
                    if mid is not None:
                        mid(h)
            if t == 0 and beside is not None:
                beside()

    def message(j, h):
        return rbuf.at[j, pl.ds(h * half, half)] if h is not None else rbuf.at[j]

    def landed(j, h):
        return r_recv.at[j if not h else n + j - 1]

    def share(target, j, h):
        return pltpu.make_async_remote_copy(
            src_ref=message(j, h), dst_ref=message(j, h), send_sem=r_send.at[target // 2, h or 0],
            recv_sem=landed(j, h), device_id={"tm": target}, device_id_type=MESH,
        )

    def forward(j, h):
        return pltpu.make_async_remote_copy(
            src_ref=message(j, h), dst_ref=message(j, h), send_sem=fwd_send.at[j if not h else 0],
            recv_sem=landed(j, h), device_id={"tm": lax.rem(me + n - 1, n)}, device_id_type=MESH,
        )

    first_targets = (3, 1)
    far_targets = range(3, n, 2)

    def each_share(act, h):
        for target in far_targets:

            @pl.when(jnp.logical_and(me > 1, me < target))
            def _():
                act(share(target, partner, h))

        @pl.when(jnp.logical_and(odd == 1, me > 1))
        def _():
            act(share(partner, partner, h))

    def start(copy):
        copy.start()

    def wait_send(copy):
        copy.wait_send()

    @pl.when(me == 0)
    def _():
        swap.wait_recv()

        def first_share(h):
            for target in first_targets:
                share(target, 1, h).start()

        interval(store_to(rbuf.at[1]), turn=M + 1, mid=first_share)
        for h in range(HALVES):
            onward(h).start()
        for z in range(zones):
            rbuf[0, z] = ubuf[z]

    prepare_coarse()

    @pl.when(jnp.logical_and(odd == 0, me > 0))
    def _():
        for z in range(zones):
            put(0, z, ubuf[z])
        swap.wait_recv()

    @pl.when(odd == 1)
    def _():
        for h in (1, 0):
            onward(h).wait_recv()
            for z in range(h * half, (h + 1) * half):
                put(0, z, carr[z])
        swap.wait_recv()

    @pl.when(me > 1)
    def _():
        def right_side(z, value):
            rbuf[partner, z] = value - pbuf[z]

        interval(right_side, lambda: propagate(0, 1, coarse_dt, store_to(pbuf)))

    early = list(range(1, parts_of[0].stop - 1))
    late = [p for p in range(pairs) if p not in early]
    late = [[p for p in late if p in parts_of[0]], [p for p in late if p not in parts_of[0]]]

    @pl.when(me == 3)
    def _():
        def second(z, value):
            rbuf[2, z] = value + rbuf[2, z]

        for h in range(HALVES):
            forward(1, h).wait_recv()
            for z in range(h * half, (h + 1) * half):
                put(0, z, rbuf[1, z])
            if h == 0:
                propagate(0, 1, coarse_dt, second, span=early)
        forward(1, None).start()
        for h in range(HALVES):
            propagate(0, 1, coarse_dt, second, span=late[h])
            each_share(start, h)

    @pl.when(me != 3)
    def _():
        each_share(start, None)

    def arrive(j, h=None):
        forward(j, h).wait_recv()

        @pl.when(jnp.logical_and(odd == 1, j < me - 1))
        def _():
            forward(j, h).start()

    @pl.when(me == 0)
    def _():
        for z in range(zones):
            put(0, z, initial_at(z))

    @pl.when(me == 1)
    def _():
        for z in range(zones):
            put(0, z, carr[z])

    @pl.when(me == 2)
    def _():
        forward(1, None).wait_recv()
        for z in range(zones):
            put(0, z, rbuf[1, z])

    for j in range(3, n - 1, 2):

        @pl.when(me > j)
        def _():
            arrive(j)

    @pl.when(me == 3)
    def _():
        for z in range(zones):
            put(0, z, rbuf[2, z])

    @pl.when(jnp.logical_or(me == 1, me == 2))
    def _():
        for h in range(HALVES):
            forward(me, h).wait_recv()

    @pl.when(me > 2)
    def _():
        forward(me, None).wait_recv()

    def corner(z, value):
        emit_out(M - 1, z, jnp.where(me > 2, value, 0.0) + rbuf[me, z])

    def finish(turn=0):
        for t in range(M - 1):
            fine_step(t, t % 2, functools.partial(emit_out, t), keep=t < M - 2, turn=turn + t + (t > 0))
            if t == 0:
                propagate(0, 1, coarse_dt, corner, turn)

    def chain(src, dst, j, span=None, turn=0):
        def emit(z, value):
            put(dst, z, value + rbuf[j, z])

        propagate(src, 1, coarse_dt, emit, turn, span)

    def begin(parity, last):
        for h in range(HALVES):
            arrive(2, h)
            for z in range(h * half, (h + 1) * half):
                put(start_x, z, rbuf[2, z])
            if h == 0:
                chain(start_x, parity, 3, early)
        if parity == 1 and not last:
            arrive(4)
        chain(start_x, parity, 3, late[0][1:] + late[1] + late[0][:1])
        turn = late[0][-1] + 1
        if parity == 1:
            chain(1, 0, 4, turn=turn)
            turn += 1
        if last:
            finish(turn)

    @pl.when(me < 4)
    def _():
        finish()

    for parity in range(2):

        @pl.when(me == 4 + parity)
        def _():
            begin(parity, True)

        @pl.when(jnp.logical_and(me > 5, odd == parity))
        def _():
            begin(parity, False)

    for left_over in range(n - 5 - n % 2, 0, -1):
        if left_over % 2 == 1:

            @pl.when(me > left_over + 4)
            def _():
                j = me - 1 - left_over

                @pl.when(jnp.logical_or(odd == 0, left_over > 1))
                def _():
                    arrive(j + odd)

                chain(0, 1, j)
                chain(1, 0, j + 1, turn=1)
                if left_over == 1:
                    finish(2)

    swap.wait_send()
    for h in range(HALVES):

        @pl.when(jnp.logical_or(hands_on, me == 0))
        def _():
            onward(h).wait_send()

        @pl.when(me == 0)
        def _():
            for target in first_targets:
                share(target, 1, h).wait_send()

        @pl.when(me == 3)
        def _():
            each_share(wait_send, h)

    @pl.when(me != 3)
    def _():
        each_share(wait_send, None)

    @pl.when(me == 3)
    def _():
        forward(1, None).wait_send()

    @pl.when(jnp.logical_and(odd == 1, me > 3))
    def _():
        for h in range(HALVES):
            forward(2, h).wait_send()

    def drain(j, _):
        forward(j, None).wait_send()
        return 0

    lax.fori_loop(3, jnp.where(odd == 1, me - 1, 3), drain, 0)


def solution(mesh):
    n = mesh.shape["tm"]

    def body(initial, forcing, fine_blocks, coarse_blocks):
        inst, slots, cells = forcing.shape
        zones, _, blk, _ = fine_blocks.shape
        blocks = cells // blk
        reps = blocks // zones
        rows = inst * reps
        assert slots == M and n > 4 and n % 2 == 0 and zones % (2 * HALVES) == 0
        pieces = 4 if zones % 4 == 0 else 1
        init_rows = initial.reshape(inst, blocks, blk).transpose(1, 0, 2).reshape(-1, blk)
        forc_rows = forcing.reshape(inst, slots, blocks, blk).transpose(0, 2, 1, 3).reshape(-1, blk)
        state = pltpu.VMEM((zones, rows, blk), jnp.float32)
        out = pl.pallas_call(
            functools.partial(kernel, n, inst, zones, reps, pieces),
            out_shape=pltpu.VMEM(forc_rows.shape, jnp.float32),
            in_specs=[pl.BlockSpec(memory_space=pltpu.HBM)] * 4,
            out_specs=pl.BlockSpec(memory_space=pltpu.VMEM),
            scratch_shapes=[
                pltpu.VMEM(init_rows.shape, jnp.float32),
                pltpu.VMEM(forc_rows.shape, jnp.float32),
                pltpu.VMEM(forc_rows.shape, jnp.float32),
                pltpu.VMEM((2,) + fine_blocks.shape, jnp.float32),
                pltpu.VMEM((2, zones, 3 * blk, 2 * blk), F8),
                pltpu.VMEM((2, zones // 2, 3 * blk, 2 * blk), F8),
                pltpu.VMEM((2, zones + 2, 2 * rows, blk), jnp.bfloat16),
                pltpu.VMEM((zones + 2, 2 * rows, blk), jnp.bfloat16),
                state,
                state,
                pltpu.VMEM((n, zones, rows, blk), jnp.float32),
                state,
                pltpu.SemaphoreType.DMA((6,)),
                pltpu.SemaphoreType.DMA((2,)),
                pltpu.SemaphoreType.DMA,
                pltpu.SemaphoreType.DMA,
                pltpu.SemaphoreType.DMA((HALVES,)),
                pltpu.SemaphoreType.DMA((HALVES,)),
                pltpu.SemaphoreType.DMA((n // 2, HALVES)),
                pltpu.SemaphoreType.DMA((n + 2,)),
                pltpu.SemaphoreType.DMA((n - 2,)),
            ],
            compiler_params=pltpu.CompilerParams(collective_id=0, has_side_effects=True),
        )(init_rows, forc_rows, fine_blocks, coarse_blocks)
        return out.reshape(inst, blocks, slots, blk).transpose(0, 2, 1, 3).reshape(forcing.shape)

    in_specs = (P("grp", None), P("grp", "tm", None), P(), P())
    out_specs = P("grp", "tm", None)
    return jax.shard_map(body, mesh=mesh, in_specs=in_specs, out_specs=out_specs, check_vma=False)
```
